256 devices in a mesh: width: 8 (over x, core), hidden: 32 (over z, y).
Axes of the slice: x: 4, y: 4, z: 8, core: 2. Of those that a mesh axis runs over, the one named last changes fastest.
Arguments:
- inputs: bfloat16 [512, 6144], P(None, 'width'), may hold values from -6 to 6
- weight_in: bfloat16 [6144, 16384], P('width', 'hidden'), may hold values from -0.078125 to 0.078125
- weight_out: bfloat16 [16384, 6144], P('hidden', 'width'), may hold values from -0.046875 to 0.046875
- gradient_in: bfloat16 [6144, 16384], P('width', 'hidden'), may hold values from -10.4 to 10.4
- gradient_out: bfloat16 [16384, 6144], P('hidden', 'width'), may hold values from -10.4 to 10.4
- left_in: bfloat16 [6144, 384], P('width'), may hold values from -5 to 7, as said below
- right_in: bfloat16 [16384, 256], P('hidden'), may hold values from -5 to 7, as said below
- left_out: bfloat16 [16384, 256], P('hidden'), may hold values from -5 to 7, as said below
- right_out: bfloat16 [6144, 384], P('width'), may hold values from -5 to 7, as said below
- damping: float32 [1], replicated, may hold values from 0.5 to 2
Outputs:
- step_in: float32 [6144, 16384], P('width', 'hidden')
- step_out: float32 [16384, 6144], P('hidden', 'width')
- res_in: float32 [6144, 16384], P('width', 'hidden')
- res_out: float32 [16384, 6144], P('hidden', 'width')
The draws below stay inside these ranges and needn't reach their ends.
Inputs may be any that keep to these rules, and one draw needn't show every extreme that they name: `left_in`: each aligned block of 384 rows is one symmetric positive definite 384 x 384 matrix. `right_in`: each aligned block of 256 rows is one symmetric positive definite 256 x 256 matrix. `left_out`: each aligned block of 256 rows is one symmetric positive definite 256 x 256 matrix. `right_out`: each aligned block of 384 rows is one symmetric positive definite 384 x 384 matrix.
All inputs are finite; a program needn't handle non-finite values.
Results may differ from the reference program's by a relative error of at most 0.025.
Values may be sent and summed in bfloat16 or wider, within the bound.
No kernel may reach another device: no remote copies, remote signals or barrier semaphores. Data moves between devices by JAX's collectives and lax.ppermute only.
A program may use at most 64 MiB of HBM per device.

```python
import math
import jax
import jax.numpy as jnp
from jax import lax

D = 6144
FF = 16384
BD = 384
BF = 256
ITERS = 2
TOKENS = 512


def block_factor(key, row_total, block_size):
    block_count = row_total // block_size
    matrix_key, diagonal_key = jax.random.split(key)
    matrix = jnp.clip(jax.random.normal(matrix_key, (block_count, block_size, block_size), jnp.float32), -3.0, 3.0)
    diagonal = jnp.exp(jax.random.uniform(diagonal_key, (block_count, block_size), jnp.float32, -0.6931472, 0.6931472))
    gram = jnp.einsum('kab,kcb->kac', matrix, matrix) * (0.5 / block_size)
    identity = jnp.eye(block_size, dtype=jnp.float32)
    blocks = gram + identity[None, :, :] * diagonal[:, :, None]
    return blocks.reshape(row_total, block_size).astype(jnp.bfloat16)


def rising_field(key, row_total, col_total, row_weight, col_weight):
    row_place = jnp.arange(row_total, dtype=jnp.float32)[:, None] / row_total
    col_place = jnp.arange(col_total, dtype=jnp.float32)[None, :] / col_total
    level = row_weight * row_place + col_weight * col_place
    noise = jnp.clip(jax.random.normal(key, (row_total, col_total), jnp.float32), -6.0, 6.0)
    scales = jnp.sqrt(1.0 + 2.0 * level)
    return (noise * scales).astype(jnp.bfloat16)


def draw_gradient_in(key, part):
    return rising_field(jax.random.fold_in(key, 21), D, FF, 0.9, 0.1)


def draw_gradient_out(key, part):
    return rising_field(jax.random.fold_in(key, 22), FF, D, 0.1, 0.9)


def draw_left_in(key, part):
    return block_factor(jax.random.fold_in(key, 11), D, BD)


def draw_right_in(key, part):
    return block_factor(jax.random.fold_in(key, 12), FF, BF)


def draw_left_out(key, part):
    return block_factor(jax.random.fold_in(key, 13), FF, BF)


def draw_right_out(key, part):
    return block_factor(jax.random.fold_in(key, 14), D, BD)


def block_levels(stream_key, extent, pieces, low, top_value):
    def one(axis_at, shards_of):
        heights = jax.random.uniform(jax.random.fold_in(jax.random.fold_in(stream_key, 6), axis_at), (shards_of,), jnp.float32, low / len(pieces), top_value / len(pieces))
        return jnp.repeat(jnp.exp(heights), extent[axis_at] // shards_of).reshape((-1,) + (1,) * (len(extent) - axis_at - 1))

    factor_of = one(*pieces[0])
    for cut in pieces[1:]:
        factor_of = factor_of * one(*cut)
    return factor_of


def normal_values(stream_key, shape, deviation, reach, shards=(), kind=jnp.bfloat16):
    values = deviation * jax.random.normal(stream_key, shape, jnp.float32)
    if shards:
        values = values * block_levels(stream_key, shape, shards, -0.22, 0.18)
    return jnp.clip(values, -reach, reach).astype(kind)


def setup_inputs(seed: int = 0) -> dict:
    streams_of = jax.random.split(jax.random.key(seed), 11)
    return {
        "inputs": normal_values(streams_of[0], (TOKENS, D), 1.0, 6.0, ((1, 8),)),
        "weight_in": normal_values(streams_of[1], (D, FF), D ** -0.5, 0.078125, ((0, 8), (1, 32))),
        "weight_out": normal_values(streams_of[2], (FF, D), FF ** -0.5, 0.046875, ((0, 32), (1, 8))),
        "gradient_in": draw_gradient_in(jax.random.fold_in(streams_of[10], 71), 0),
        "gradient_out": draw_gradient_out(jax.random.fold_in(streams_of[10], 71), 0),
        "left_in": draw_left_in(jax.random.fold_in(streams_of[10], 71), 0),
        "right_in": draw_right_in(jax.random.fold_in(streams_of[10], 71), 0),
        "left_out": draw_left_out(jax.random.fold_in(streams_of[10], 71), 0),
        "right_out": draw_right_out(jax.random.fold_in(streams_of[10], 71), 0),
        "damping": jnp.clip(jnp.exp(jax.random.uniform(streams_of[9], (1,), jnp.float32, math.log(0.5), math.log(2.0))), 0.5, 2.0),
    }


HIGHEST_PRECISION = lax.Precision.HIGHEST


def activate(pre_act):
    normal_cdf = 0.5 * (1.0 + lax.erf(pre_act * 0.7071067811865476))
    activation = (pre_act * normal_cdf).astype(jnp.bfloat16)
    slopes = (normal_cdf + pre_act * jnp.exp(-0.5 * pre_act * pre_act) * 0.3989422804014327).astype(jnp.bfloat16)
    return activation, slopes


def left_apply(blocks, matrix, block_size):
    row_total, col_total = matrix.shape
    stacked = blocks.astype(jnp.float32).reshape(row_total // block_size, block_size, block_size)
    shaped = matrix.reshape(row_total // block_size, block_size, col_total)
    product = jnp.einsum("kab,kbc->kac", stacked, shaped, precision=HIGHEST_PRECISION)
    return product.reshape(row_total, col_total)


def right_apply(blocks, matrix, block_size):
    row_total, col_total = matrix.shape
    stacked = blocks.astype(jnp.float32).reshape(col_total // block_size, block_size, block_size)
    shaped = matrix.reshape(row_total, col_total // block_size, block_size)
    product = jnp.einsum("rkb,kbc->rkc", shaped, stacked, precision=HIGHEST_PRECISION)
    return product.reshape(row_total, col_total)


def reference(inputs, weight_in, weight_out, gradient_in, gradient_out, left_in, right_in, left_out, right_out, damping):
    pre_act = jnp.dot(inputs, weight_in, preferred_element_type=jnp.float32)
    activation, slopes = activate(pre_act)
    damper = damping[0]

    def precondition(first_part, second_part):
        first_new = right_apply(right_in, left_apply(left_in, first_part, BD), BF)
        second_new = right_apply(right_out, left_apply(left_out, second_part, BF), BD)
        return first_new, second_new

    def curvature(vector_in, vector_out):
        tan_pre = jnp.dot(inputs, vector_in.astype(jnp.bfloat16), preferred_element_type=jnp.float32)
        tan_act = (slopes * tan_pre).astype(jnp.bfloat16)
        out_sum = jnp.dot(tan_act, weight_out, preferred_element_type=jnp.float32)
        out_sum = out_sum + jnp.dot(activation, vector_out.astype(jnp.bfloat16), preferred_element_type=jnp.float32)
        errors = (out_sum / TOKENS).astype(jnp.bfloat16)
        back_act = jnp.dot(errors, weight_out.T, preferred_element_type=jnp.float32)
        back_pre = (slopes * back_act).astype(jnp.bfloat16)
        image_in = jnp.dot(inputs.T, back_pre, preferred_element_type=jnp.float32) + damper * vector_in
        image_out = jnp.dot(activation.T, errors, preferred_element_type=jnp.float32) + damper * vector_out
        return image_in, image_out

    res_in = gradient_in.astype(jnp.float32)
    res_out = gradient_out.astype(jnp.float32)
    step_in = jnp.zeros_like(res_in)
    step_out = jnp.zeros_like(res_out)
    precond_in, precond_out = precondition(res_in, res_out)
    norm_now = jnp.sum(res_in * precond_in) + jnp.sum(res_out * precond_out)
    search_in, search_out = precond_in, precond_out
    for iteration in range(ITERS):
        image_in, image_out = curvature(search_in, search_out)
        step_size = norm_now / (jnp.sum(search_in * image_in) + jnp.sum(search_out * image_out))
        step_in = step_in + step_size * search_in
        step_out = step_out + step_size * search_out
        res_in = res_in - step_size * image_in
        res_out = res_out - step_size * image_out
        if iteration + 1 < ITERS:
            precond_in, precond_out = precondition(res_in, res_out)
            norm_next = jnp.sum(res_in * precond_in) + jnp.sum(res_out * precond_out)
            momentum = norm_next / norm_now
            search_in = precond_in + momentum * search_in
            search_out = precond_out + momentum * search_out
            norm_now = norm_next
    return step_in, step_out, res_in, res_out
```

```python
import functools

import jax
import jax.numpy as jnp
from jax import lax
from jax.experimental import pallas as pl
from jax.experimental.pallas import tpu as pltpu
from jax.sharding import Mesh
from jax.sharding import PartitionSpec as P

BD = 384
BF = 256
WIDTH = ("width_0", "width_1")
HIDDEN = ("hidden_0", "hidden_1")
F32 = jnp.float32
BF16 = jnp.bfloat16


def cut_along(array, dim, size):
    shape = array.shape
    tiles = array.reshape(*shape[:dim], size, shape[dim] // size, *shape[dim + 1 :])
    return jnp.moveaxis(tiles, dim, 0)


def sent(array, axis):
    size = lax.axis_size(axis)
    return lax.all_to_all(cut_along(array, 0, size), axis, 0, 0, tiled=True)


def summed(tiles):
    return jnp.sum(tiles.astype(F32), axis=0)


def copied(array, axis):
    copies = jnp.broadcast_to(array, (lax.axis_size(axis), *array.shape))
    return lax.all_to_all(copies, axis, split_axis=0, concat_axis=0, tiled=True)


def collect(array, axis):
    tiles = copied(array, axis)
    return tiles.reshape(tiles.shape[0] * tiles.shape[1], *tiles.shape[2:])


def activate(pre_act):
    normal_cdf = 0.5 * (1.0 + lax.erf(pre_act * 0.7071067811865476))
    activation = (pre_act * normal_cdf).astype(BF16)
    slopes = (normal_cdf + pre_act * jnp.exp(-0.5 * pre_act * pre_act) * 0.3989422804014327).astype(BF16)
    return activation, slopes


def mm(a, b):
    return lax.dot_general(a, b, (((1,), (0,)), ((), ())), preferred_element_type=F32)


def mm_tn(a, b):
    return lax.dot_general(a, b, (((0,), (0,)), ((), ())), preferred_element_type=F32)


def mm_nt(a, b):
    return lax.dot_general(a, b, (((1,), (1,)), ((), ())), preferred_element_type=F32)


def right_blocks(matrix, blocks, size):
    parts = [
        mm(matrix[:, k : k + size], blocks[k : k + size, :]) for k in range(0, matrix.shape[1], size)
    ]
    return jnp.concatenate(parts, axis=1)


def left_blocks(blocks, matrix, size):
    parts = [
        mm(blocks[k : k + size, :], matrix[k : k + size, :]) for k in range(0, matrix.shape[0], size)
    ]
    return jnp.concatenate(parts, axis=0)


def precondition(left, matrix, right, left_size, right_size):
    return right_blocks(left_blocks(left, matrix, left_size).astype(BF16), right, right_size)


def lanes(array):
    total = jnp.sum(array, axis=0, keepdims=True)
    return sum(total[:, k : k + 128] for k in range(0, total.shape[1], 128))


def rows_of(*parts):
    blank = jnp.zeros((8 - len(parts), 128), F32)
    return jnp.concatenate([*parts, blank], axis=0)


def whole(kernel, outs, *args, flops=0, name=None):
    shapes = [jax.ShapeDtypeStruct(shape, dtype) for shape, dtype in outs]
    nbytes = sum(a.size * a.dtype.itemsize for a in args) + sum(s.size * s.dtype.itemsize for s in shapes)
    return pl.pallas_call(
        kernel,
        out_shape=shapes,
        name=name,
        cost_estimate=pl.CostEstimate(flops=flops, bytes_accessed=nbytes, transcendentals=0),
        compiler_params=pltpu.CompilerParams(vmem_limit_bytes=40 * 1024 * 1024),
    )(*args)


def start_in(x, gi, li, ri, z_ref, tan_ref, sums_ref):
    g = gi[...]
    z = precondition(li[...], g, ri[...], BD, BF)
    z_ref[...] = z
    tan_ref[...] = mm(x[...], z.astype(BF16)).astype(BF16)
    sums_ref[...] = rows_of(lanes(g.astype(F32) * z), lanes(z * z))


def start_out(go, lo, ro, sums_in, z_ref, sums_ref):
    g = go[...]
    z = precondition(lo[...], g, ro[...], BF, BD)
    z_ref[...] = z
    sums_ref[...] = sums_in[...] + rows_of(lanes(g.astype(F32) * z), lanes(z * z))


def second_order(x, z, li, ri, both_ref):
    again = precondition(li[...], z[...].astype(BF16), ri[...], BD, BF).astype(BF16)
    inputs = x[...]
    scaled = jnp.concatenate(
        [mm(inputs[:, k : k + BD], li[k : k + BD, :]) for k in range(0, inputs.shape[1], BD)], axis=1
    )
    both_ref[:, :512] = mm_nt(scaled.astype(BF16), inputs).astype(BF16)
    both_ref[:, 512:] = mm(inputs, again).astype(BF16)


def first_error(act, slopes, tan, wo, z, error_ref):
    tan_act = (slopes[...].astype(F32) * tan[...].astype(F32)).astype(BF16)
    error_ref[...] = (mm(tan_act, wo[...]) + mm(act[...], z[...].astype(BF16))).astype(BF16)


def total_of(sums):
    return jnp.sum(jnp.sum(sums[...], axis=0), axis=1, keepdims=True)


def first_size(sums, damper, tokens):
    total = total_of(sums)
    return total[0:1] / (tokens * total[2:3] + damper * total[1:2])


def error_sums(error, sums, out_ref):
    e = error[...].astype(F32)
    zero = jnp.zeros((1, 128), F32)
    out_ref[...] = jnp.sum(sums[...], axis=0) + rows_of(zero, zero, lanes(e * e))


def middle_out(tokens, act, error, z, go, lo, ro, sums, damping, r_ref, z_ref, p_ref, sums_ref):
    damper = damping[0]
    size = first_size(sums, damper, tokens)
    z0 = z[...]
    q = mm_tn(act[...], error[...]) + damper * z0
    r = go[...].astype(F32) - size * q
    z1 = precondition(lo[...], r.astype(BF16), ro[...], BF, BD)
    r_ref[...] = r
    z_ref[...] = z1
    p_ref[...] = mm(act[...], z1.astype(BF16))
    sums_ref[...] = rows_of(lanes(r * z1), lanes(z1 * z1), lanes(z1 * z0))


def second_error(tokens, both, back, ri, tan, slopes, wo, part, sums, damping, error_ref):
    damper = damping[0]
    size = first_size(sums, damper, tokens)
    moved = right_blocks(mm(both[:, :512], back[...]).astype(BF16), ri[...], BF)
    tan1 = tan[...].astype(F32) - size * (moved + damper * both[:, 512:].astype(F32))
    tan_act = (slopes[...].astype(F32) * tan1).astype(BF16)
    error_ref[...] = (mm(tan_act, wo[...]) + part[...]).astype(BF16)


def middle_in(tokens, x, back, z, gi, li, ri, sums, sums_out, damping, r_ref, z_ref, sums_ref):
    damper = damping[0]
    size = first_size(sums, damper, tokens)
    z0 = z[...]
    q = mm_tn(x[...], back[...]) + damper * z0
    r = gi[...].astype(F32) - size * q
    z1 = precondition(li[...], r.astype(BF16), ri[...], BD, BF)
    r_ref[...] = r
    z_ref[...] = z1
    sums_ref[...] = sums_out[...] + rows_of(lanes(r * z1), lanes(z1 * z1), lanes(z1 * z0))


def error_sums_2(error0, error1, sums, out_ref):
    e0, e1 = error0[...].astype(F32), error1[...].astype(F32)
    zero = jnp.zeros((1, 128), F32)
    out_ref[...] = jnp.sum(sums[...], axis=0) + rows_of(
        zero, zero, zero, lanes(e0 * e0), lanes(e1 * e0), lanes(e1 * e1)
    )


def last_sizes(tokens, first, last, damper):
    before, now = total_of(first), total_of(last)
    rz0, zz0 = before[0:1], before[1:2]
    size0 = rz0 / (tokens * before[2:3] + damper * zz0)
    rz1, zz1, zp = now[0:1], now[1:2], now[2:3]
    momentum = rz1 / rz0
    errors = now[5:6] + 2.0 * momentum * now[4:5] + momentum * momentum * now[3:4]
    norms = zz1 + 2.0 * momentum * zp + momentum * momentum * zz0
    return size0, momentum, rz1 / (tokens * errors + damper * norms)


def finish_out(tokens, act, error0, error1, z0, z1, r1, first, last, damping, step_ref, res_ref):
    damper = damping[0]
    size0, momentum, size1 = last_sizes(tokens, first, last, damper)
    start = z0[...]
    search = z1[...] + momentum * start
    error = (error1[...].astype(F32) + momentum * error0[...].astype(F32)).astype(BF16)
    step_ref[...] = size0 * start + size1 * search
    res_ref[...] = r1[...] - size1 * (mm_tn(act[...], error) + damper * search)


def finish_in(tokens, x, back0, back1, z0, z1, r1, first, last, damping, step_ref, res_ref):
    damper = damping[0]
    size0, momentum, size1 = last_sizes(tokens, first, last, damper)
    start = z0[...]
    search = z1[...] + momentum * start
    back = (back1[...].astype(F32) + momentum * back0[...].astype(F32)).astype(BF16)
    step_ref[...] = size0 * start + size1 * search
    res_ref[...] = r1[...] - size1 * (mm_tn(x[...], back) + damper * search)


def with_scalars(kernel, n_in, scalar_at):
    return kernel


def body(x, wi, wo, gi, go, li, ri, lo, ro, damping):
    tokens = float(x.shape[0])
    n, d = x.shape
    f = wi.shape[1]
    in_, out_ = (d, f), (f, d)
    tile = ((8, 128), F32)

    pre_tiles = sent(mm(x, wi).astype(BF16), WIDTH)
    z0_in, tan_part, sums = whole(
        start_in, [(in_, F32), ((n, f), BF16), tile], x, gi, li, ri, flops=2**30, name="start_in"
    )
    tan_tiles = sent(tan_part, WIDTH)
    z0_out, sums = whole(
        start_out, [(out_, F32), tile], go, lo, ro, sums, flops=2**29, name="start_out"
    )
    sums0 = copied(sums, HIDDEN)
    (both_part,) = whole(
        second_order, [((n, 2 * f), BF16)], x, z0_in, li, ri, flops=2**31, name="second_order"
    )

    pre_share = summed(pre_tiles)
    pre_act = collect(pre_share.astype(BF16), WIDTH)
    tan = collect(summed(tan_tiles).astype(BF16), WIDTH)
    _, slopes_share = activate(pre_share)
    act, slopes = activate(pre_act.astype(F32))

    (part,) = whole(
        first_error, [((n, d), BF16)], act, slopes, tan, wo, z0_out, flops=2**30, name="first_error"
    )
    error_tiles = sent(part, HIDDEN)
    both_tiles = sent(both_part, WIDTH)
    both = collect(summed(both_tiles).astype(BF16), WIDTH)
    error0 = collect((summed(error_tiles) / tokens).astype(BF16), HIDDEN)

    def back_of(error):
        tiles = sent(mm_nt(error, wo).astype(BF16), WIDTH)
        return collect((slopes_share.astype(F32) * summed(tiles)).astype(BF16), WIDTH)

    (sums,) = whole(error_sums, [tile], error0, sums0, flops=2**20, name="error_sums")
    first = copied(sums, WIDTH)
    back0 = back_of(error0)

    smem = pl.BlockSpec(memory_space=pltpu.SMEM)
    r1_out, z1_out, part_out, sums_out = whole_s(
        functools.partial(middle_out, tokens),
        [(out_, F32), (out_, F32), ((n, d), F32), tile],
        act, error0, z0_out, go, lo, ro, first, damping, flops=3 * 2**29, name="middle_out",
    )
    (part,) = whole_s(
        functools.partial(second_error, tokens),
        [((n, d), BF16)],
        both, back0, ri, tan, slopes, wo, part_out, first, damping, flops=2**30, name="second_error",
    )
    error_tiles = sent(part, HIDDEN)
    r1_in, z1_in, sums = whole_s(
        functools.partial(middle_in, tokens),
        [(in_, F32), (in_, F32), tile],
        x, back0, z0_in, gi, li, ri, first, sums_out, damping, flops=2**30, name="middle_in",
    )
    sums1 = copied(sums, HIDDEN)
    error1 = collect((summed(error_tiles) / tokens).astype(BF16), HIDDEN)
    (sums,) = whole(error_sums_2, [tile], error0, error1, sums1, flops=2**20, name="error_sums_2")
    last = copied(sums, WIDTH)
    back1 = back_of(error1)
    step_out, res_out = whole_s(
        functools.partial(finish_out, tokens),
        [(out_, F32), (out_, F32)],
        act, error0, error1, z0_out, z1_out, r1_out, first, last, damping, flops=2**29, name="finish_out",
    )
    step_in, res_in = whole_s(
        functools.partial(finish_in, tokens),
        [(in_, F32), (in_, F32)],
        x, back0, back1, z0_in, z1_in, r1_in, first, last, damping, flops=2**29, name="finish_in",
    )
    return step_in, step_out, res_in, res_out


def whole_s(kernel, outs, *args, flops=0, name=None):
    shapes = [jax.ShapeDtypeStruct(shape, dtype) for shape, dtype in outs]
    nbytes = sum(a.size * a.dtype.itemsize for a in args) + sum(s.size * s.dtype.itemsize for s in shapes)
    vmem = pl.BlockSpec(memory_space=pltpu.VMEM)
    return pl.pallas_call(
        kernel,
        out_shape=shapes,
        in_specs=[vmem] * (len(args) - 1) + [pl.BlockSpec(memory_space=pltpu.SMEM)],
        out_specs=[vmem] * len(shapes),
        name=name,
        cost_estimate=pl.CostEstimate(flops=flops, bytes_accessed=nbytes, transcendentals=0),
        compiler_params=pltpu.CompilerParams(vmem_limit_bytes=40 * 1024 * 1024),
    )(*args)


def solution(mesh):
    finer = Mesh(mesh.devices.reshape(4, 2, 8, 4), ("width_0", "width_1", "hidden_0", "hidden_1"))
    return jax.shard_map(
        body,
        mesh=finer,
        in_specs=(
            P(None, WIDTH),
            P(WIDTH, HIDDEN),
            P(HIDDEN, WIDTH),
            P(WIDTH, HIDDEN),
            P(HIDDEN, WIDTH),
            P(WIDTH, None),
            P(HIDDEN, None),
            P(HIDDEN, None),
            P(WIDTH, None),
            P(),
        ),
        out_specs=(P(WIDTH, HIDDEN), P(HIDDEN, WIDTH), P(WIDTH, HIDDEN), P(HIDDEN, WIDTH)),
        check_vma=False,
    )
```

```python
import functools

import jax
import jax.numpy as jnp
from jax import lax
from jax.experimental import pallas as pl
from jax.experimental.pallas import tpu as pltpu
from jax.sharding import Mesh
from jax.sharding import PartitionSpec as P


BD = 384
BF = 256
WIDTH = ("width_0", "width_1")
HIDDEN = ("hidden_0", "hidden_1")
F32 = jnp.float32
BF16 = jnp.bfloat16


def cut_along(array, dim, size):
    shape = array.shape
    tiles = array.reshape(*shape[:dim], size, shape[dim] // size, *shape[dim + 1 :])
    return jnp.moveaxis(tiles, dim, 0)


def sent(array, axis):
    size = lax.axis_size(axis)
    return lax.all_to_all(cut_along(array, 0, size), axis, 0, 0, tiled=True)


def summed(tiles):
    return jnp.sum(tiles.astype(F32), axis=0)


def copied(array, axis):
    copies = jnp.broadcast_to(array, (lax.axis_size(axis), *array.shape))
    return lax.all_to_all(copies, axis, split_axis=0, concat_axis=0, tiled=True)


def collect(array, axis):
    tiles = copied(array, axis)
    return tiles.reshape(tiles.shape[0] * tiles.shape[1], *tiles.shape[2:])


def shifted(array, axis, by):
    size = lax.axis_size(axis)
    return lax.ppermute(array, axis, [(k, (k + by) % size) for k in range(size)])


def neighbours(array, axis):
    return [array] + [shifted(array, axis, by) for by in range(1, lax.axis_size(axis))]


def activate(pre_act):
    normal_cdf = 0.5 * (1.0 + lax.erf(pre_act * 0.7071067811865476))
    activation = (pre_act * normal_cdf).astype(BF16)
    slopes = (normal_cdf + pre_act * jnp.exp(-0.5 * pre_act * pre_act) * 0.3989422804014327).astype(BF16)
    return activation, slopes


def mm(a, b):
    return lax.dot_general(a, b, (((1,), (0,)), ((), ())), preferred_element_type=F32)


def mm_tn(a, b):
    return lax.dot_general(a, b, (((0,), (0,)), ((), ())), preferred_element_type=F32)


def mm_nt(a, b):
    return lax.dot_general(a, b, (((1,), (1,)), ((), ())), preferred_element_type=F32)


def right_blocks(matrix, blocks, size):
    parts = [
        mm(matrix[:, k : k + size], blocks[k : k + size, :]) for k in range(0, matrix.shape[1], size)
    ]
    return jnp.concatenate(parts, axis=1)


def left_blocks(blocks, matrix, size):
    parts = [
        mm(blocks[k : k + size, :], matrix[k : k + size, :]) for k in range(0, matrix.shape[0], size)
    ]
    return jnp.concatenate(parts, axis=0)


def precondition(left, matrix, right, left_size, right_size):
    return right_blocks(left_blocks(left, matrix, left_size).astype(BF16), right, right_size)


def lanes(array):
    total = jnp.sum(array, axis=0, keepdims=True)
    return sum(total[:, k : k + 128] for k in range(0, total.shape[1], 128))


def stacked(parts, rows):
    row = lax.broadcasted_iota(jnp.int32, (rows, 128), 0)
    total = jnp.zeros((rows, 128), F32)
    for k, part in enumerate(parts):
        total = jnp.where(row == k, jnp.broadcast_to(part, (rows, 128)), total)
    return total


def packed(sums, count):
    parts = []
    for k in range(count):
        rest = sums[k : k + 1, :]
        for _ in range(3):
            piece = rest.astype(BF16).astype(F32)
            parts.append(piece)
            rest = rest - piece
    return stacked(parts, 16).astype(BF16)


def unpacked(tiles, count):
    total = jnp.sum(tiles.astype(F32), axis=0)
    return [
        total[3 * k : 3 * k + 1] + total[3 * k + 1 : 3 * k + 2] + total[3 * k + 2 : 3 * k + 3]
        for k in range(count)
    ]


def scalars(tiles, count):
    return [jnp.sum(row, axis=1, keepdims=True) for row in unpacked(tiles, count)]


VMEM_LIMIT = 60 * 1024 * 1024


class Far:
    def __init__(self, array):
        self.array = array


def whole(kernel, outs, args, smem=(), flops=0, scratch=(), far_outs=0, by_hand=False):
    shapes = [jax.ShapeDtypeStruct(shape, dtype) for shape, dtype in outs]
    far = [isinstance(a, Far) for a in args]
    arrays = [a.array if isinstance(a, Far) else a for a in args]
    near = pl.BlockSpec(memory_space=pltpu.VMEM)
    away, small = pl.BlockSpec(memory_space=pltpu.HBM), pl.BlockSpec(memory_space=pltpu.SMEM)
    buffers = [pltpu.VMEM(a.shape, a.dtype) for a, f in zip(arrays, far) if f]
    targets = [pltpu.VMEM(s.shape, s.dtype) for s in shapes[len(shapes) - far_outs :]]
    n_in, n_far = len(arrays), len(buffers)
    sems = [pltpu.SemaphoreType.DMA((max(n_far + far_outs, 1),))]

    def run(*refs):
        ins, small_refs = refs[:n_in], refs[n_in : n_in + len(smem)]
        out_refs = refs[n_in + len(smem) : n_in + len(smem) + len(shapes)]
        rest = refs[n_in + len(smem) + len(shapes) :]
        held, ready, extra, sem = rest[:n_far], rest[n_far : n_far + far_outs], rest[n_far + far_outs : -1], rest[-1]
        copies, used = [], []
        for ref, is_far in zip(ins, far):
            if is_far:
                k = len(copies)
                copies.append(pltpu.make_async_copy(ref, held[k], sem.at[k]))
                copies[-1].start()
                used.append(held[k])
            else:
                used.append(ref)
        for copy in copies:
            copy.wait()
        if far_outs:
            near_outs, far_refs = out_refs[: len(shapes) - far_outs], out_refs[len(shapes) - far_outs :]
            writes = [
                pltpu.make_async_copy(ready[k], far_refs[k], sem.at[n_far + k]) for k in range(far_outs)
            ]
            if by_hand:
                kernel(*used, *small_refs, *near_outs, *ready, *extra, writes)
            else:
                kernel(*used, *small_refs, *near_outs, *ready, *extra)
                for write in writes:
                    write.start()
            for write in writes:
                write.wait()
        else:
            kernel(*used, *small_refs, *out_refs, *extra)

    nbytes = sum(a.size * a.dtype.itemsize for a in arrays) + sum(s.size * s.dtype.itemsize for s in shapes)
    return pl.pallas_call(
        run,
        out_shape=shapes,
        in_specs=[away if f else near for f in far] + [small] * len(smem),
        out_specs=[near] * (len(shapes) - far_outs) + [away] * far_outs,
        scratch_shapes=[*buffers, *targets, *scratch, *sems],
        cost_estimate=pl.CostEstimate(flops=flops, bytes_accessed=nbytes, transcendentals=0),
        compiler_params=pltpu.CompilerParams(vmem_limit_bytes=VMEM_LIMIT),
    )(*arrays, *smem)


def start_in(x, wi, gi, li, ri, part_ref, sums_ref, z_ref):
    g = gi[...]
    inputs = x[...]
    half = wi.shape[1]
    part_ref[:, :half] = mm(inputs, wi[...]).astype(BF16)
    z = precondition(li[...], g, ri[...], BD, BF)
    near = z.astype(BF16)
    part_ref[:, half:] = mm(inputs, near).astype(BF16)
    z_ref[...] = near
    sums_ref[...] = stacked([lanes(g.astype(F32) * z), lanes(z * z)], 8)


def start_out(go, lo, ro, sums_in, sums_ref, z_ref):
    g = go[...]
    z = precondition(lo[...], g, ro[...], BF, BD)
    z_ref[...] = z.astype(BF16)
    sums_ref[...] = sums_in[...] + stacked([lanes(g.astype(F32) * z), lanes(z * z)], 8)


def second_order(x, z, li, ri, both_ref):
    again = precondition(li[...], z[...], ri[...], BD, BF).astype(BF16)
    inputs = x[...]
    scaled = jnp.concatenate(
        [mm(inputs[:, k : k + BD], li[k : k + BD, :]) for k in range(0, inputs.shape[1], BD)], axis=1
    )
    tokens = inputs.shape[0]
    both_ref[:, :tokens] = mm_nt(scaled.astype(BF16), inputs).astype(BF16)
    both_ref[:, tokens:] = mm(inputs, again).astype(BF16)


def cut_pair(both, other, place, *pieces):
    rows = pieces[0].shape[0]
    for by, piece in enumerate(pieces):
        here = pl.ds(pl.multiple_of(lax.rem(place[0] + by, len(pieces)) * rows, rows), rows)
        piece[...] = (both[here, :].astype(F32) + other[here, :].astype(F32)).astype(BF16)


def add_pieces(a, b, c, d, total_ref):
    total_ref[...] = (
        a[...].astype(F32) + b[...].astype(F32) + c[...].astype(F32) + d[...].astype(F32)
    ).astype(BF16)


def first_error(shared, wo, z, part_ref, act_ref, slopes_ref, tan_ref, direct_ref):
    half = shared.shape[1] // 2
    act, slopes = activate(shared[:, :half].astype(F32))
    act_ref[...] = act
    slopes_ref[...] = slopes
    tan_ref[...] = shared[:, half:]
    tan_act = (slopes.astype(F32) * shared[:, half:].astype(F32)).astype(BF16)
    direct = mm(act, z[...]).astype(BF16)
    direct_ref[...] = direct
    part_ref[...] = (mm(tan_act, wo[...]) + direct.astype(F32)).astype(BF16)


def share_error(tokens, count, tiles, sums, copies_ref):
    total = jnp.sum(tiles[...].astype(F32), axis=0) / tokens
    width = total.shape[1]
    copies = copies_ref.shape[0]
    copies_ref[:, :, :width] = jnp.broadcast_to(total.astype(BF16)[None], (copies, *total.shape))
    extra = packed(sums[...], count)
    copies_ref[:, :, width:] = jnp.broadcast_to(extra[None], (copies, *extra.shape))


def spread_back(error, wo_refs, me, part_ref):
    rows = error.reshape(error.shape[0] * error.shape[1], error.shape[2])
    for by, wo in enumerate(wo_refs):
        back = mm_nt(rows, wo[...]).astype(BF16)
        part_ref[:, lax.rem(me + (len(wo_refs) - by), len(wo_refs))] = back.reshape(
            error.shape[0], error.shape[1], back.shape[1]
        )


def first_back(found, w0, w1, w2, w3, place, part_ref, sums_ref, error_ref):
    width = error_ref.shape[2]
    error = found[:, :, :width]
    spread_back(error, (w0, w1, w2, w3), place[0], part_ref)
    error_ref[...] = error
    e = error.astype(F32).reshape(-1, width)
    sums_ref[...] = stacked([*unpacked(found[:, :, width:], 2), lanes(e * e)], 8)


def second_back(found, before, w0, w1, w2, w3, place, part_ref, sums_ref, error_ref):
    width = error_ref.shape[2]
    error = found[:, :, :width]
    spread_back(error, (w0, w1, w2, w3), place[0], part_ref)
    error_ref[...] = error
    e1 = error.astype(F32).reshape(-1, width)
    e0 = before[...].astype(F32).reshape(-1, width)
    sums_ref[...] = stacked([*unpacked(found[:, :, width:], 3), lanes(e1 * e0), lanes(e1 * e1)], 8)


def share_back(count, tiles, sums, copies_ref):
    total = jnp.sum(tiles[...].astype(F32), axis=0).astype(BF16)
    extra = packed(sums[...], count)
    width = total.shape[2]
    copies_ref[:, :, :, :width] = jnp.broadcast_to(total[None], (copies_ref.shape[0], *total.shape))
    copies_ref[:, :, :, width:] = jnp.broadcast_to(
        extra[None, None], (copies_ref.shape[0], copies_ref.shape[1], *extra.shape)
    )


def in_order(pieces, me, order_ref):
    for by, piece in enumerate(pieces):
        order_ref[:, lax.rem(me + (len(pieces) - by), len(pieces))] = piece[...]
    shape = order_ref.shape
    return order_ref[...].reshape(shape[0] * shape[1] * shape[2], shape[3])


def image_out(act, e0, e1, e2, e3, z, lo, ro, damping, place, q_ref, move_ref, order_ref):
    error = in_order((e0, e1, e2, e3), place[0], order_ref)
    q = mm_tn(act[...], error) + damping[0] * z[...].astype(F32)
    near = q.astype(BF16)
    q_ref[...] = near
    moved = precondition(lo[...], near, ro[...], BF, BD)
    move_ref[...] = mm(act[...], moved.astype(BF16)).astype(BF16)


def back_products(found, slopes):
    width = slopes.shape[1]
    share = found[:, :, :width].reshape(slopes.shape)
    return (slopes[...].astype(F32) * share.astype(F32)).astype(BF16)


def second_error(
    tokens, b0, b1, b2, b3, found, ri, tan0, slopes, wo, direct, move, damping, place, part_ref, back_ref, known_ref, both
):
    damper = damping[0]
    pieces, rows = (b0, b1, b2, b3), b0.shape[0]
    for by, piece in enumerate(pieces):
        at = lax.rem(place[0] + (len(pieces) - by), len(pieces)) * rows
        both[pl.ds(pl.multiple_of(at, rows), rows), :] = piece[...]
    half = slopes.shape[1]
    back = back_products(found, slopes)
    back_ref[...] = back
    rz, zz, ee = scalars(found[:, :, half:], 3)
    size = rz / (tokens * ee + damper * zz)
    known_ref[...] = stacked([size, rz, zz, ee], 8)
    cols = both.shape[0]
    change = right_blocks(mm(both[:, :cols], back).astype(BF16), ri[...], BF)
    tan = tan0[...].astype(F32) - size * (change + damper * both[:, cols:].astype(F32))
    tan_act = (slopes[...].astype(F32) * tan).astype(BF16)
    part_ref[...] = (mm(tan_act, wo[...]) + (direct[...].astype(F32) - size * move[...].astype(F32))).astype(BF16)


def middle_out(go, q, z, lo, ro, known, sums_ref, r_ref, z_ref):
    size = known[0:1, 0:1]
    r = go[...].astype(F32) - size * q[...].astype(F32)
    near = r.astype(BF16)
    z1 = precondition(lo[...], near, ro[...], BF, BD)
    r_ref[...] = near
    z_ref[...] = z1.astype(BF16)
    sums_ref[...] = stacked([lanes(r * z1), lanes(z1 * z1), lanes(z1 * z[...].astype(F32))], 8)


def middle_in(x, back, z, gi, li, ri, known, sums, damping, sums_ref, r_ref, z_ref, q_ref):
    damper = damping[0]
    size = known[0:1, 0:1]
    z0 = z[...].astype(F32)
    q = mm_tn(x[...], back[...]) + damper * z0
    q_ref[...] = q.astype(BF16)
    r = gi[...].astype(F32) - size * q
    near = r.astype(BF16)
    z1 = precondition(li[...], near, ri[...], BD, BF)
    r_ref[...] = near
    z_ref[...] = z1.astype(BF16)
    sums_ref[...] = sums[...] + stacked([lanes(r * z1), lanes(z1 * z1), lanes(z1 * z0)], 8)


def last_image_out(act, e0, e1, e2, e3, z, damping, place, q_ref, order_ref):
    error = in_order((e0, e1, e2, e3), place[0], order_ref)
    q_ref[...] = (mm_tn(act[...], error) + damping[0] * z[...].astype(F32)).astype(BF16)


def last_sizes(tokens, known, last, damper, width):
    size0, rz0, zz0, ee0 = (known[k : k + 1, 0:1] for k in range(4))
    rz1, zz1, zp, ep, ee1 = scalars(last[:, :, width:], 5)
    momentum = rz1 / rz0
    errors = ee1 + momentum * (2.0 * ep + momentum * ee0)
    norms = zz1 + momentum * (2.0 * zp + momentum * zz0)
    return size0, momentum, rz1 / (tokens * errors + damper * norms)


def finish(tokens, x, slopes, known, last, z0, z1, r1, q0, y0, y1, s1, p0, p1, damping, *outs):
    step_in, step_out, res_out, res_in, writes = outs
    damper = damping[0]
    size0, momentum, size1 = last_sizes(tokens, known, last, damper, slopes.shape[1])
    both_sizes = size0 + size1 * momentum
    step_in[...] = both_sizes * z0[...].astype(F32) + size1 * z1[...].astype(F32)
    writes[0].start()
    step_out[...] = both_sizes * y0[...].astype(F32) + size1 * y1[...].astype(F32)
    writes[1].start()
    image = p1[...].astype(F32) + momentum * p0[...].astype(F32)
    res_out[...] = s1[...].astype(F32) - size1 * image
    writes[2].start()
    q1 = mm_tn(x[...], back_products(last, slopes)) + damper * z1[...].astype(F32)
    res_in[...] = r1[...].astype(F32) - size1 * (q1 + momentum * q0[...].astype(F32))
    writes[3].start()


def body(x, wi, wo, gi, go, li, ri, lo, ro, damping):
    n, d = x.shape
    f = wi.shape[1]
    tokens = float(n)
    along, across = lax.axis_size("hidden_0"), lax.axis_size("hidden_1")
    wide = lax.axis_size(WIDTH)
    rows = n // (along * across)
    in_, out_, tile = ((d, f), BF16), ((f, d), BF16), ((8, 128), F32)
    place = jnp.reshape(lax.axis_index("hidden_1"), (1,))
    chip = jnp.reshape(lax.axis_index("width_0"), (1,))
    chips = lax.axis_size("width_0")
    order = [pltpu.VMEM((along, across, rows, d), BF16)]
    call = functools.partial

    def exchange_error(part, sums, count):
        tiles = sent(part, HIDDEN)
        (copies,) = whole(
            call(share_error, tokens, count), [((along, rows, d + 128), BF16)], (tiles, sums), flops=2**20
        )
        return lax.all_to_all(copies, "hidden_0", 0, 0, tiled=True)

    def exchange_back(part, sums, count):
        tiles = lax.all_to_all(part, WIDTH, 0, 0, tiled=True)
        (copies,) = whole(call(share_back, count), [((wide, across, rows, f + 128), BF16)], (tiles, sums), flops=2**20)
        copies = copies.reshape(wide * across, rows, f + 128)
        return lax.all_to_all(copies, (*WIDTH, "hidden_1"), 0, 0, tiled=True)

    part, sums, z0_in = whole(
        start_in, [((n, 2 * f), BF16), tile, in_], (Far(x), Far(wi), Far(gi), Far(li), Far(ri)), flops=2**31, far_outs=1
    )
    tiles = sent(part, WIDTH)
    rows_out = neighbours(wo, "hidden_1")
    sums, z0_out = whole(start_out, [tile, out_], (Far(go), Far(lo), Far(ro), sums), flops=2**29, far_outs=1)
    (both,) = whole(second_order, [((n, n + f), BF16)], (Far(x), Far(z0_in), Far(li), Far(ri)), flops=2**31, far_outs=1)
    share = summed(tiles).astype(BF16)
    shared = collect(share, WIDTH)
    other = shifted(both, "width_1", 1)
    part, act, slopes, tan0, direct = whole(
        first_error,
        [((n, d), BF16), ((n, f), BF16), ((n, f), BF16), ((n, f), BF16), ((n, d), BF16)],
        (shared, Far(wo), Far(z0_out)),
        flops=2**31,
        far_outs=4,
    )
    pieces = whole(
        cut_pair, [((n // chips, n + f), BF16)] * chips, (Far(both), Far(other)), (chip,), flops=2**21, far_outs=chips
    )
    found = exchange_error(part, sums, 2)
    pieces = [pieces[0]] + [shifted(pieces[by], "width_0", by) for by in range(1, chips)]
    (both,) = whole(add_pieces, [((n // chips, n + f), BF16)], pieces, flops=2**20)
    pieces = neighbours(both, "width_0")
    part_shape = ((wide, across, rows, f), BF16)
    error_shape = ((along, rows, d), BF16)
    far_rows = [Far(w) for w in rows_out]
    part, sums, error0 = whole(
        first_back, [part_shape, tile, error_shape], (found, *far_rows), (place,), 2**30, far_outs=1
    )
    errors = neighbours(error0, "hidden_1")
    first = exchange_back(part, sums, 3)
    q0_out, move = whole(
        image_out,
        [out_, ((n, d), BF16)],
        (Far(act), *[Far(e) for e in errors], Far(z0_out), Far(lo), Far(ro)),
        (damping, place),
        2**31,
        order,
        far_outs=2,
    )
    part, back, known = whole(
        call(second_error, tokens),
        [((n, d), BF16), ((n, f), BF16), tile],
        (*[Far(p) for p in pieces], first, Far(ri), Far(tan0), Far(slopes), Far(wo), Far(direct), Far(move)),
        (damping, chip),
        2**30,
        [pltpu.VMEM((n, n + f), BF16)],
        far_outs=2,
    )
    sums, r1_out, z1_out = whole(
        middle_out,
        [tile, out_, out_],
        (Far(go), Far(q0_out), Far(z0_out), Far(lo), Far(ro), Far(known)),
        flops=2**29,
        far_outs=2,
    )
    sums, r1_in, z1_in, q0_in = whole(
        middle_in,
        [tile, in_, in_, in_],
        (Far(x), Far(back), Far(z0_in), Far(gi), Far(li), Far(ri), Far(known), sums),
        (damping,),
        2**30,
        far_outs=3,
    )
    found = exchange_error(part, sums, 3)
    part, sums, error1 = whole(
        second_back, [part_shape, tile, error_shape], (found, Far(error0), *far_rows), (place,), 2**30, far_outs=1
    )
    errors = neighbours(error1, "hidden_1")
    last = exchange_back(part, sums, 5)
    (q1_out,) = whole(
        last_image_out,
        [out_],
        (Far(act), *[Far(e) for e in errors], Far(z1_out)),
        (damping, place),
        2**29,
        order,
        far_outs=1,
    )
    parts = (z0_in, z1_in, r1_in, q0_in, z0_out, z1_out, r1_out, q0_out, q1_out)
    in_, out_ = ((d, f), F32), ((f, d), F32)
    step_in, step_out, res_out, res_in = whole(
        call(finish, tokens),
        [in_, out_, out_, in_],
        (Far(x), Far(slopes), Far(known), last, *[Far(p) for p in parts]),
        (damping,),
        2**29,
        far_outs=4,
        by_hand=True,
    )
    return step_in, step_out, res_in, res_out


def solution(mesh):
    finer = Mesh(mesh.devices.reshape(4, 2, 8, 4), ("width_0", "width_1", "hidden_0", "hidden_1"))
    return jax.shard_map(
        body,
        mesh=finer,
        in_specs=(
            P(None, WIDTH),
            P(WIDTH, HIDDEN),
            P(HIDDEN, WIDTH),
            P(WIDTH, HIDDEN),
            P(HIDDEN, WIDTH),
            P(WIDTH, None),
            P(HIDDEN, None),
            P(HIDDEN, None),
            P(WIDTH, None),
            P(),
        ),
        out_specs=(P(WIDTH, HIDDEN), P(HIDDEN, WIDTH), P(WIDTH, HIDDEN), P(HIDDEN, WIDTH)),
        check_vma=False,
    )
```
